32 devices in a mesh: groups: 2 (over y), cand: 4 (over z), mp: 4 (over x, core).
Axes of the slice: x: 2, y: 2, z: 4, core: 2. Of those that a mesh axis runs over, the one named last changes fastest.
Arguments:
- user_feats: bfloat16 [8, 4096], P(('groups', 'cand')), parts along dimension 0, may hold values from -6 to 6
- user_slot: int32 [2], P('groups'), parts along dimension 0, may hold values from 0 to 3, as said below
- cand_pool: bfloat16 [512, 4096], P('groups'), parts along dimension 0, may hold values from -6 to 6
- cand_ids: int32 [2, 64], P('groups'), parts along dimension 0, may hold values from 0 to 255
- first_weight: bfloat16 [8192, 8192], P('mp', 'cand'), may hold values from -0.0625 to 0.0625
- first_bias: float32 [8192], P('cand'), may hold values from -5 to 5
- second_weight: bfloat16 [8192, 8192], P('cand', 'mp'), may hold values from -0.0625 to 0.0625
- second_bias: float32 [8192], P('mp'), may hold values from -5 to 5
- third_weight: bfloat16 [8192, 8192], P('mp', 'cand'), may hold values from -0.0625 to 0.0625
- third_bias: float32 [8192], P('cand'), may hold values from -5 to 5
- score_weight: bfloat16 [8192], P('cand'), may hold values from -0.0625 to 0.0625
Outputs:
- crossed: bfloat16 [128, 8192], P(('groups', 'mp'), 'cand'), parts along dimension 0
- logits: float32 [128], P(('groups', 'mp')), parts along dimension 0
The draws below stay inside these ranges and needn't reach their ends.
There are 2 independent parts, one for each index of `groups`. The reference program is written for one: setup_inputs(seed, part) draws one part's arguments, and reference() takes and returns one part's arrays. A program takes and returns all parts, laid end to end along the dimension named above; an argument that names none is the same for every part. Nothing has to cross between parts.
Inputs may be any that keep to these rules, and one draw needn't show every extreme that they name: `user_slot`: the users' slots are distinct.
All inputs are finite; a program needn't handle non-finite values.
Results may differ from the reference program's by a relative error of at most 0.022.
Values may be sent and summed in bfloat16 or wider, within the bound.
A program may use at most 64 MiB of HBM per device.

```python
import jax
import jax.numpy as jnp
from jax import lax

DH = 4096
D = 8192
POOL = 256
CANDS = 64
USERS = 1
SLOTS = 4
ROWS = 64
N_CAND = 4


def draw_user_slot(key, part):
    pairs = jax.random.permutation(jax.random.fold_in(key, 11), SLOTS // 2)[:USERS].astype(jnp.int32)
    bits = jax.random.randint(jax.random.fold_in(key, 12), (USERS,), 0, 2).astype(jnp.int32)
    first_bit = (jnp.asarray(part).astype(jnp.int32) % 2).astype(jnp.int32)
    bits = bits.at[0].set(first_bit)
    return (2 * pairs + bits).astype(jnp.int32)


def with_ends(drawn, key, low, largest):
    longest = drawn.shape.index(max(drawn.shape))
    spots = []
    for shift in (0, 1):
        where = [jax.random.randint(jax.random.fold_in(key, axis), (), 0, length) for axis, length in enumerate(drawn.shape)]
        where[longest] = (where[longest] + shift) % drawn.shape[longest]
        spots.append(tuple(where))
    return drawn.at[spots[0]].set(low).at[spots[1]].set(largest)


def block_scale(rng, dims, split, smallest, largest):
    def one(dim, blocks):
        steps = jax.random.uniform(jax.random.fold_in(jax.random.fold_in(rng, 6), dim), (blocks,), jnp.float32, smallest / len(split), largest / len(split))
        return jnp.repeat(jnp.exp(steps), dims[dim] // blocks).reshape((-1,) + (1,) * (len(dims) - dim - 1))

    level = one(*split[0])
    for cut in split[1:]:
        level = level * one(*cut)
    return level


def gaussian(key, shape, scale, limit, pieces=(), held_as=jnp.bfloat16):
    array = scale * jax.random.normal(key, shape, jnp.float32)
    if pieces:
        array = array * block_scale(key, shape, pieces, -0.22, 0.18)
    return jnp.clip(array, -limit, limit).astype(held_as)


def setup_inputs(seed: int = 0, part: int = 0) -> dict:
    key_list = jax.random.split(jax.random.key(seed), 12)
    part_splits = jax.random.split(jax.random.fold_in(key_list[11], part), 12)
    return {
        "user_feats": gaussian(part_splits[0], (SLOTS, DH), 1.0, 6.0, ((0, 4),)),
        "user_slot": draw_user_slot(jax.random.fold_in(jax.random.fold_in(key_list[11], part), 71), part),
        "cand_pool": gaussian(part_splits[2], (POOL, DH), 1.0, 6.0),
        "cand_ids": with_ends(jax.random.randint(part_splits[3], (USERS, CANDS), 0, POOL), jax.random.fold_in(part_splits[3], 1), 0, POOL - 1).astype(jnp.int32),
        "first_weight": gaussian(key_list[4], (D, D), D ** -0.5, 0.0625, ((0, 4), (1, 4))),
        "first_bias": gaussian(key_list[5], (D,), 1.0, 5.0, ((0, 4),), jnp.float32),
        "second_weight": gaussian(key_list[6], (D, D), D ** -0.5, 0.0625, ((0, 4), (1, 4))),
        "second_bias": gaussian(key_list[7], (D,), 1.0, 5.0, ((0, 4),), jnp.float32),
        "third_weight": gaussian(key_list[8], (D, D), D ** -0.5, 0.0625, ((0, 4), (1, 4))),
        "third_bias": gaussian(key_list[9], (D,), 1.0, 5.0, ((0, 4),), jnp.float32),
        "score_weight": gaussian(key_list[10], (D,), D ** -0.5, 0.0625, ((0, 4),)),
    }


def reference(user_feats, user_slot, cand_pool, cand_ids, first_weight, first_bias, second_weight, second_bias, third_weight, third_bias, score_weight):
    user_rows = jnp.repeat(user_feats[user_slot], CANDS, axis=0)
    pool_rows = cand_pool[cand_ids.reshape(-1)]
    base = jnp.concatenate([user_rows, pool_rows], axis=1)
    first_sum = jnp.dot(base, first_weight, preferred_element_type=jnp.float32)
    cross_one = (base * (first_sum + first_bias) + base).astype(jnp.bfloat16)
    block = D // N_CAND
    second_sum = jnp.zeros((ROWS, D), jnp.float32)
    for piece in range(N_CAND):
        term = jnp.dot(cross_one[:, piece * block:(piece + 1) * block], second_weight[piece * block:(piece + 1) * block], preferred_element_type=jnp.float32)
        term = lax.optimization_barrier(term.astype(jnp.bfloat16))
        second_sum = second_sum + term.astype(jnp.float32)
    cross_two = (base * (second_sum + second_bias) + cross_one).astype(jnp.bfloat16)
    third_sum = jnp.dot(cross_two, third_weight, preferred_element_type=jnp.float32)
    cross_three = base * (third_sum + third_bias) + cross_two
    logits = jnp.sum(cross_three * score_weight.astype(jnp.float32), axis=1)
    return cross_three.astype(jnp.bfloat16), logits
```

```python
import jax
import jax.numpy as jnp
from jax import lax
from jax.experimental import pallas as pl
from jax.experimental.pallas import tpu as pltpu
from jax.sharding import PartitionSpec as P

MESH = pl.DeviceIdType.MESH
F32 = jnp.float32
BF16 = jnp.bfloat16


def reverse_bits(value, bits):
    out = 0
    for _ in range(bits):
        out = 2 * out + value % 2
        value //= 2
    return out


def make_kernel(n_mp, n_cand, shapes):
    rows, per_user, users, slots_each, half_width, pool_count, feat, col, n1, n2 = shapes
    cw1, cw2 = col // n1, feat // n2
    bits = n_mp.bit_length() - 1
    block = rows // n_mp
    ratio = feat // col
    group = n_mp * n_cand

    def kernel(
        user_ref, slot_ref, pool_hbm, ids_ref, w1_hbm, b1_ref, w2_hbm, b2_ref, w3_hbm, b3_ref, score_ref,
        out_ref, logit_ref,
        slots, pool_v, w1_v, w2_v, w3_v, onehot, base_mp, base_col,
        acc1, send1, recv1, cross1, acc2, q_send, l_recv, r_recv, l_send, r_send, x3, acc3, send3, recv3, q_rows, q_all,
        w_sem, user_ss, user_rs, a_ss, a_rs, g_ss, g_rs, l_ss, l_rs, r_ss, r_rs, c_ss, c_rs, q_ss, q_rs,
    ):
        i = lax.axis_index("mp")
        j = lax.axis_index("cand")
        me = i * n_cand + j
        pending = []

        def remote(src, dst, ss, rs, where):
            return pltpu.make_async_remote_copy(
                src_ref=src, dst_ref=dst, send_sem=ss, recv_sem=rs, device_id=where, device_id_type=MESH
            )

        pool_copy = pltpu.make_async_copy(pool_hbm, pool_v, w_sem.at[0])
        w1_copies = [
            pltpu.make_async_copy(w1_hbm.at[:, pl.ds(c * cw1, cw1)], w1_v.at[c], w_sem.at[1 + c]) for c in range(n1)
        ]
        w2_copies = [
            pltpu.make_async_copy(w2_hbm.at[pl.ds(c * cw1, cw1), :], w2_v.at[pl.ds(c * cw1, cw1), :], w_sem.at[1 + n1 + c])
            for c in range(n1)
        ]
        w3_copies = [
            pltpu.make_async_copy(w3_hbm.at[pl.ds(c * cw2, cw2), :], w3_v.at[pl.ds(c * cw2, cw2), :], w_sem.at[1 + 2 * n1 + c])
            for c in range(n2)
        ]
        pool_copy.start()
        for copy in w1_copies:
            copy.start()

        barrier = pltpu.get_barrier_semaphore()

        def greet(d, carry):
            peer = lax.rem(me + d, group)
            pl.semaphore_signal(
                barrier, inc=1, device_id={"mp": peer // n_cand, "cand": lax.rem(peer, n_cand)}, device_id_type=MESH
            )
            return carry

        lax.fori_loop(1, group, greet, 0)
        pl.semaphore_wait(barrier, group - 1)

        def user_copy(d):
            return remote(
                user_ref, slots.at[j], user_ss.at[d - 1], user_rs.at[j], {"cand": lax.rem(j + d, n_cand)}
            )

        for d in range(1, n_cand):
            user_copy(d).start()
        slots[j] = user_ref[...]

        for u in range(users):
            hot = (
                lax.broadcasted_iota(jnp.int32, (pool_count, per_user), 0) == ids_ref[u : u + 1, :]
            ).astype(F32).T
            for p in range(n_mp):
                first = reverse_bits(p, bits) * block
                if first // per_user == u:
                    off = first % per_user
                    onehot[p * block : (p + 1) * block, :] = hot[off : off + block].astype(BF16)

        def from_pool(dst, index, width):
            @pl.when(index >= half_width // width)
            def _():
                for c in range(0, width, 256):
                    start = pl.multiple_of(index * width - half_width + c, 128)
                    dst[:, c : c + 256] = jnp.dot(
                        onehot[...], pool_v[:, pl.ds(start, 256)], preferred_element_type=F32
                    ).astype(BF16)

        def from_user(dst, index, width):
            @pl.when(index < half_width // width)
            def _():
                start = pl.multiple_of(index * width, 128)
                for p in range(n_mp):
                    slot = slot_ref[(reverse_bits(p, bits) * block) // per_user]
                    row = slots[slot // slots_each, :, pl.ds(start, width)].astype(F32)
                    if slots_each > 1:
                        pick = lax.broadcasted_iota(jnp.int32, row.shape, 0) == lax.rem(slot, slots_each)
                        row = jnp.sum(jnp.where(pick, row, 0.0), axis=0, keepdims=True)
                    dst[p * block : (p + 1) * block, :] = jnp.broadcast_to(row, (block, width)).astype(BF16)

        pool_copy.wait()
        from_pool(base_mp, i, feat)
        from_pool(base_col, j, col)
        for d in range(1, n_cand):
            k = lax.rem(j - d + n_cand, n_cand)
            remote(user_ref, slots.at[k], user_ss.at[d - 1], user_rs.at[k], {"cand": k}).wait_recv()
        from_user(base_mp, i, feat)
        from_user(base_col, j, col)

        def bit_of(b):
            return lax.rem(i // (1 << b), 2)

        def partner(b):
            return i + (1 << b) * (1 - 2 * bit_of(b))

        lows = [0]
        for b in range(bits):
            lows.append(lows[b] + bit_of(b) * (rows >> (b + 1)))

        def seg(b):
            size = rows >> b
            if b == 0:
                return pl.ds(0, rows)
            return pl.ds(pl.multiple_of(lows[b], size), size)

        def other(b):
            size = rows >> (b + 1)
            low = lows[b] + (1 - bit_of(b)) * size
            return pl.ds(pl.multiple_of(low, size), size)

        last = bits - 1

        def scatter_copy(c, b):
            rng = other(b) if b < last else seg(b)
            size = rows >> min(b + 1, last)
            return remote(
                send1.at[c, rng, :], recv1.at[b, c, pl.ds(0, size), :], a_ss.at[b, c], a_rs.at[b, c], {"mp": partner(b)}
            )

        def gather_copy(c, b):
            return remote(
                cross1.at[c, seg(b + 1), :], cross1.at[c, seg(b + 1), :], g_ss.at[b, c], g_rs.at[b, c], {"mp": partner(b)}
            )

        def gather_wait(c, b):
            remote(
                cross1.at[c, other(b), :], cross1.at[c, other(b), :], g_ss.at[b, c], g_rs.at[b, c], {"mp": partner(b)}
            ).wait_recv()

        def stage_a(c):
            w1_copies[c].wait()
            term = jnp.dot(base_mp[...], w1_v[c], preferred_element_type=F32)
            acc1[c] = term
            send1[c] = term.astype(BF16)
            copy = scatter_copy(c, 0)
            copy.start()
            pending.append(copy)

        def stage_b(c):
            for b in range(last):
                scatter_copy(c, b).wait_recv()
                size = rows >> (b + 1)
                term = acc1[c, seg(b + 1), :] + recv1[b, c, 0:size, :].astype(F32)
                if b + 1 < last:
                    acc1[c, seg(b + 1), :] = term
                send1[c, seg(b + 1), :] = term.astype(BF16)
                copy = scatter_copy(c, b + 1)
                copy.start()
                pending.append(copy)

        def stage_c(c):
            scatter_copy(c, last).wait_recv()
            size = rows >> last
            total = send1[c, seg(last), :].astype(F32) + recv1[last, c, 0:size, :].astype(F32)
            cols = slice(c * cw1, (c + 1) * cw1)
            base = base_col[seg(last), cols].astype(F32)
            cross1[c, seg(last), :] = (base * (total + b1_ref[:, cols]) + base).astype(BF16)
            if last > 0:
                copy = gather_copy(c, last - 1)
                copy.start()
                pending.append(copy)

        def line_copy(n, right, first):
            src = (q_send if first else (l_send if right else r_send)).at[n]
            if right:
                return remote(src, l_recv.at[n], l_ss.at[n], l_rs.at[n], {"cand": j + 1})
            return remote(src, r_recv.at[n], r_ss.at[n], r_rs.at[n], {"cand": j - 1})

        def stage_d(c):
            for b in range(last - 1, -1, -1):
                gather_wait(c, b)
                if b > 0:
                    copy = gather_copy(c, b - 1)
                    copy.start()
                    pending.append(copy)
            w2_copies[c].wait()
            for n in range(n2):
                cols = slice(n * cw2, (n + 1) * cw2)
                term = jnp.dot(
                    cross1[c], w2_v[c * cw1 : (c + 1) * cw1, cols], preferred_element_type=F32
                )
                if c > 0:
                    term = acc2[:, cols] + term
                if c < n1 - 1:
                    acc2[:, cols] = term
                    continue
                owner = (j == i * ratio + (n * cw2) // col).astype(F32)
                inner = (n * cw2) % col
                carried = cross1[inner // cw1, :, inner % cw1 : inner % cw1 + cw2].astype(F32)
                term = base_mp[:, cols].astype(F32) * (term + owner * b2_ref[:, cols]) + owner * carried
                q_send[n] = term.astype(BF16)

                @pl.when(j == 0)
                def _():
                    line_copy(n, True, True).start()

                @pl.when(j == n_cand - 1)
                def _():
                    line_copy(n, False, True).start()

        order = []
        for s in range(n1 + 1):
            if s < n1:
                order.append((stage_a, s))
            if s >= 1:
                order.append((stage_b, s - 1))
        for s in range(n1 + 1):
            if s < n1:
                order.append((stage_c, s))
            if s >= 1:
                order.append((stage_d, s - 1))
        started = False
        for stage, c in order:
            stage(c)
            if stage is stage_a and c == n1 - 1:
                for copy in w2_copies:
                    copy.start()
            if stage is stage_c and not started:
                started = True
                for copy in w3_copies:
                    copy.start()

        def forward(n, right):
            came = (l_recv if right else r_recv)[n].astype(F32)
            (l_send if right else r_send)[n] = (came + q_send[n].astype(F32)).astype(BF16)
            line_copy(n, right, False).start()

        def take(n, right):
            if right:
                remote(l_send.at[n], l_recv.at[n], l_ss.at[n], l_rs.at[n], {"cand": j}).wait_recv()
            else:
                remote(r_send.at[n], r_recv.at[n], r_ss.at[n], r_rs.at[n], {"cand": j}).wait_recv()

        def third(n):
            w3_copies[n].wait()
            for p in range(n1):
                cols = slice(p * cw1, (p + 1) * cw1)
                term = jnp.dot(
                    x3[:, n * cw2 : (n + 1) * cw2], w3_v[n * cw2 : (n + 1) * cw2, cols], preferred_element_type=F32
                )
                if n > 0:
                    term = acc3[:, cols] + term
                acc3[:, cols] = term

        skew = min(3, n2)
        near_left = j < (n_cand + 1) // 2
        inner_device = jnp.logical_and(j > 0, j < n_cand - 1)
        for s in range(n2 + skew):
            if s < n2:
                @pl.when(jnp.logical_and(inner_device, near_left))
                def _():
                    take(s, True)
                    forward(s, True)

                @pl.when(jnp.logical_and(inner_device, jnp.logical_not(near_left)))
                def _():
                    take(s, False)
                    forward(s, False)

            n = s - skew
            if n < 0:
                continue

            @pl.when(jnp.logical_and(inner_device, near_left))
            def _():
                take(n, False)
                forward(n, False)

            @pl.when(jnp.logical_and(inner_device, jnp.logical_not(near_left)))
            def _():
                take(n, True)
                forward(n, True)

            cols = slice(n * cw2, (n + 1) * cw2)

            @pl.when(inner_device)
            def _():
                x3[:, cols] = (
                    q_send[n].astype(F32) + l_recv[n].astype(F32) + r_recv[n].astype(F32)
                ).astype(BF16)

            @pl.when(j == 0)
            def _():
                take(n, False)
                x3[:, cols] = (q_send[n].astype(F32) + r_recv[n].astype(F32)).astype(BF16)

            @pl.when(j == n_cand - 1)
            def _():
                take(n, True)
                x3[:, cols] = (q_send[n].astype(F32) + l_recv[n].astype(F32)).astype(BF16)

            third(n)

        def last_copy(c, b):
            size = rows >> (b + 1)
            return remote(
                send3.at[c, other(b), :], recv3.at[b, c, pl.ds(0, size), :], c_ss.at[b, c], c_rs.at[b, c], {"mp": partner(b)}
            )

        owner = (i == j // ratio).astype(F32)
        lanes = jnp.zeros((rows, 128), F32)
        for c in range(n1):
            cols = slice(c * cw1, (c + 1) * cw1)
            if ratio == 1:
                carried = x3[:, cols]
            else:
                carried = x3[:, pl.ds(pl.multiple_of(lax.rem(j, ratio) * col + c * cw1, 128), cw1)]
            term = (
                base_col[:, cols].astype(F32) * (acc3[:, cols] + owner * b3_ref[:, cols])
                + owner * carried.astype(F32)
            )
            acc3[:, cols] = term
            send3[c] = term.astype(BF16)
            copy = last_copy(c, 0)
            copy.start()
            pending.append(copy)
            scored = term * score_ref[:, cols].astype(F32)
            for k in range(0, cw1, 128):
                lanes = lanes + scored[:, k : k + 128]
        q_rows[...] = jnp.zeros_like(q_rows)
        q_rows[0:rows, :] = lanes
        q_all[me] = jnp.sum(q_rows[...].T, axis=0, keepdims=True)

        def q_copy(d):
            peer = lax.rem(me + d, group)
            return remote(
                q_all.at[me], q_all.at[me], q_ss.at[d], q_rs.at[me],
                {"mp": peer // n_cand, "cand": lax.rem(peer, n_cand)},
            )

        def q_start(d, carry):
            q_copy(d).start()
            return carry

        lax.fori_loop(1, group, q_start, 0)

        for b in range(bits):
            for c in range(n1):
                cols = slice(c * cw1, (c + 1) * cw1)
                last_copy(c, b).wait_recv()
                size = rows >> (b + 1)
                term = acc3[seg(b + 1), cols] + recv3[b, c, 0:size, :].astype(F32)
                if b + 1 < bits:
                    acc3[seg(b + 1), cols] = term
                    send3[c, seg(b + 1), :] = term.astype(BF16)
                    copy = last_copy(c, b + 1)
                    copy.start()
                    pending.append(copy)
                else:
                    out_ref[:, cols] = term.astype(BF16)

        def q_wait(d, carry):
            k = lax.rem(me - d + group, group)
            remote(q_all.at[k], q_all.at[k], q_ss.at[d], q_rs.at[k], {"cand": j}).wait_recv()
            return carry

        lax.fori_loop(1, group, q_wait, 0)
        total = jnp.sum(q_all[...], axis=0)
        for k in range(n_mp):
            p = reverse_bits(k, bits)

            @pl.when(i == k)
            def _():
                logit_ref[...] = total[:, p * block : (p + 1) * block]

        for copy in pending:
            copy.wait_send()
        for d in range(1, n_cand):
            user_copy(d).wait_send()

        def q_sent(d, carry):
            q_copy(d).wait_send()
            return carry

        lax.fori_loop(1, group, q_sent, 0)
        for n in range(n2):
            @pl.when(j < n_cand - 1)
            def _():
                line_copy(n, True, False).wait_send()

            @pl.when(j > 0)
            def _():
                line_copy(n, False, False).wait_send()

    return kernel


def solution(mesh):
    n_mp, n_cand = mesh.shape["mp"], mesh.shape["cand"]

    def body(
        user_feats, user_slot, cand_pool, cand_ids, first_weight, first_bias,
        second_weight, second_bias, third_weight, third_bias, score_weight,
    ):
        slots_each, half_width = user_feats.shape
        users, per_user = cand_ids.shape
        rows = users * per_user
        pool_count = cand_pool.shape[0]
        feat, col = first_weight.shape
        n1 = max(1, col // 512)
        n2 = max(1, feat // 256)
        cw1, cw2 = col // n1, feat // n2
        bits = n_mp.bit_length() - 1
        block = rows // n_mp
        group = n_mp * n_cand
        shapes = (rows, per_user, users, slots_each, half_width, pool_count, feat, col, n1, n2)
        vmem = pl.BlockSpec(memory_space=pltpu.VMEM)
        smem = pl.BlockSpec(memory_space=pltpu.SMEM)
        hbm = pl.BlockSpec(memory_space=pl.ANY)
        dma = pltpu.SemaphoreType.DMA
        exchange = rows >> (1 if bits > 1 else 0)
        crossed, logits = pl.pallas_call(
            make_kernel(n_mp, n_cand, shapes),
            out_shape=(
                jax.ShapeDtypeStruct((block, col), BF16),
                jax.ShapeDtypeStruct((1, block), F32),
            ),
            in_specs=[vmem, smem, hbm, vmem, hbm, vmem, hbm, vmem, hbm, vmem, vmem],
            out_specs=(vmem, vmem),
            scratch_shapes=[
                pltpu.VMEM((n_cand, slots_each, half_width), BF16),
                pltpu.VMEM((pool_count, half_width), BF16),
                pltpu.VMEM((n1, feat, cw1), BF16),
                pltpu.VMEM((col, feat), BF16),
                pltpu.VMEM((feat, col), BF16),
                pltpu.VMEM((rows, pool_count), BF16),
                pltpu.VMEM((rows, feat), BF16),
                pltpu.VMEM((rows, col), BF16),
                pltpu.VMEM((n1, rows, cw1), F32),
                pltpu.VMEM((n1, rows, cw1), BF16),
                pltpu.VMEM((bits, n1, exchange, cw1), BF16),
                pltpu.VMEM((n1, rows, cw1), BF16),
                pltpu.VMEM((rows, feat), F32),
                pltpu.VMEM((n2, rows, cw2), BF16),
                pltpu.VMEM((n2, rows, cw2), BF16),
                pltpu.VMEM((n2, rows, cw2), BF16),
                pltpu.VMEM((n2, rows, cw2), BF16),
                pltpu.VMEM((n2, rows, cw2), BF16),
                pltpu.VMEM((rows, feat), BF16),
                pltpu.VMEM((rows, col), F32),
                pltpu.VMEM((n1, rows, cw1), BF16),
                pltpu.VMEM((bits, n1, rows // 2, cw1), BF16),
                pltpu.VMEM((max(rows, 128), 128), F32),
                pltpu.VMEM((group, 1, max(rows, 128)), F32),
                dma((1 + 2 * n1 + n2,)),
                dma((n_cand,)),
                dma((n_cand,)),
                dma((bits, n1)),
                dma((bits, n1)),
                dma((bits, n1)),
                dma((bits, n1)),
                dma((n2,)),
                dma((n2,)),
                dma((n2,)),
                dma((n2,)),
                dma((bits, n1)),
                dma((bits, n1)),
                dma((group,)),
                dma((group,)),
            ],
            compiler_params=pltpu.CompilerParams(
                collective_id=0, has_side_effects=True, vmem_limit_bytes=60000 * 1024
            ),
        )(
            user_feats, user_slot, cand_pool, cand_ids, first_weight, first_bias.reshape(1, -1),
            second_weight, second_bias.reshape(1, -1), third_weight, third_bias.reshape(1, -1),
            score_weight.reshape(1, -1),
        )
        return crossed, logits.reshape(-1)

    in_specs = (
        P(("groups", "cand"), None),
        P("groups"),
        P("groups", None),
        P("groups", None),
        P("mp", "cand"),
        P("cand"),
        P("cand", "mp"),
        P("mp"),
        P("mp", "cand"),
        P("cand"),
        P("cand"),
    )
    out_specs = (P(("groups", "mp"), "cand"), P(("groups", "mp")))
    return jax.shard_map(body, mesh=mesh, in_specs=in_specs, out_specs=out_specs, check_vma=False)
```

```python
import jax
import jax.numpy as jnp
from jax import lax
from jax.experimental import pallas as pl
from jax.experimental.pallas import tpu as pltpu
from jax.sharding import PartitionSpec as P

MESH = pl.DeviceIdType.MESH
F32 = jnp.float32
BF16 = jnp.bfloat16


def reverse_bits(value, bits):
    out = 0
    for _ in range(bits):
        out = 2 * out + value % 2
        value //= 2
    return out


def hand_on(crossed_ref, logit_ref, crossed_hbm, logit_hbm, sem):
    copies = [
        pltpu.make_async_copy(crossed_ref, crossed_hbm, sem.at[0]),
        pltpu.make_async_copy(logit_ref, logit_hbm, sem.at[1]),
    ]
    for copy in copies:
        copy.start()
    for copy in copies:
        copy.wait()


def make_kernel(n_mp, n_cand, shapes):
    rows, per_user, users, slots_each, half_width, pool_count, feat, col, n1, n2 = shapes
    cw1, cw2 = col // n1, feat // n2
    bits = n_mp.bit_length() - 1
    block = rows // n_mp
    ratio = feat // col
    group = n_mp * n_cand

    def kernel(
        user_hbm, slot_ref, pool_hbm, ids_hbm, w1_hbm, b1_hbm, w2_hbm, b2_hbm, w3_hbm, b3_hbm, score_hbm,
        out_ref, logit_ref,
        user_ref, ids_ref, b1_ref, b2_ref, b3_ref, score_ref, small_sem, slots, pool_v, w1_v, w2_v, w3_v, onehot, base_mp, base_col,
        acc1, send1, recv1, cross1, acc2, q_send, l_recv, r_recv, l_send, r_send, x3, acc3, send3, recv3, q_rows, q_all,
        w_sem, user_ss, user_rs, a_ss, a_rs, g_ss, g_rs, l_ss, l_rs, r_ss, r_rs, c_ss, c_rs, q_ss, q_rs,
    ):
        i = lax.axis_index("mp")
        j = lax.axis_index("cand")
        me = i * n_cand + j
        pending = []

        def remote(src, dst, ss, rs, where):
            return pltpu.make_async_remote_copy(
                src_ref=src, dst_ref=dst, send_sem=ss, recv_sem=rs, device_id=where, device_id_type=MESH
            )

        small_copies = [
            pltpu.make_async_copy(src, dst, small_sem.at[k])
            for k, (src, dst) in enumerate(
                (
                    (user_hbm, user_ref), (ids_hbm, ids_ref), (b1_hbm, b1_ref),
                    (b2_hbm, b2_ref), (b3_hbm, b3_ref), (score_hbm, score_ref),
                )
            )
        ]
        for copy in small_copies:
            copy.start()
        barrier = pltpu.get_barrier_semaphore()

        def greet(d, carry):
            peer = lax.rem(me + d, group)
            pl.semaphore_signal(
                barrier, inc=1, device_id={"mp": peer // n_cand, "cand": lax.rem(peer, n_cand)}, device_id_type=MESH
            )
            return carry

        lax.fori_loop(1, group, greet, 0)

        pool_copy = pltpu.make_async_copy(pool_hbm, pool_v, w_sem.at[0])
        w1_copies = [
            pltpu.make_async_copy(w1_hbm.at[:, pl.ds(c * cw1, cw1)], w1_v.at[c], w_sem.at[1 + c]) for c in range(n1)
        ]
        w2_copies = [
            pltpu.make_async_copy(w2_hbm.at[pl.ds(c * cw1, cw1), :], w2_v.at[pl.ds(c * cw1, cw1), :], w_sem.at[1 + n1 + c])
            for c in range(n1)
        ]
        w3_copies = [
            pltpu.make_async_copy(w3_hbm.at[pl.ds(c * cw2, cw2), :], w3_v.at[pl.ds(c * cw2, cw2), :], w_sem.at[1 + 2 * n1 + c])
            for c in range(n2)
        ]
        pool_copy.start()
        for copy in w1_copies:
            copy.start()

        small_copies[0].wait()
        pl.semaphore_wait(barrier, group - 1)

        def user_copy(d):
            return remote(
                user_ref, slots.at[j], user_ss.at[d - 1], user_rs.at[j], {"cand": lax.rem(j + d, n_cand)}
            )

        for d in range(1, n_cand):
            user_copy(d).start()
        slots[j] = user_ref[...]
        small_copies[1].wait()

        for u in range(users):
            hot = (
                lax.broadcasted_iota(jnp.int32, (pool_count, per_user), 0) == ids_ref[u : u + 1, :]
            ).astype(F32).T
            for p in range(n_mp):
                first = reverse_bits(p, bits) * block
                if first // per_user == u:
                    off = first % per_user
                    onehot[p * block : (p + 1) * block, :] = hot[off : off + block].astype(BF16)

        def from_pool(dst, index, width):
            @pl.when(index >= half_width // width)
            def _():
                for c in range(0, width, 256):
                    start = pl.multiple_of(index * width - half_width + c, 128)
                    dst[:, c : c + 256] = jnp.dot(
                        onehot[...], pool_v[:, pl.ds(start, 256)], preferred_element_type=F32
                    ).astype(BF16)

        def from_user(dst, index, width):
            @pl.when(index < half_width // width)
            def _():
                start = pl.multiple_of(index * width, 128)
                for p in range(n_mp):
                    slot = slot_ref[(reverse_bits(p, bits) * block) // per_user]
                    row = slots[slot // slots_each, :, pl.ds(start, width)].astype(F32)
                    if slots_each > 1:
                        pick = lax.broadcasted_iota(jnp.int32, row.shape, 0) == lax.rem(slot, slots_each)
                        row = jnp.sum(jnp.where(pick, row, 0.0), axis=0, keepdims=True)
                    dst[p * block : (p + 1) * block, :] = jnp.broadcast_to(row, (block, width)).astype(BF16)

        def from_all_users():
            for d in range(1, n_cand):
                k = lax.rem(j - d + n_cand, n_cand)
                remote(user_ref, slots.at[k], user_ss.at[d - 1], user_rs.at[k], {"cand": k}).wait_recv()

        pool_copy.wait()
        from_pool(base_mp, i, feat)
        user_side = i < half_width // feat

        @pl.when(user_side)
        def _():
            from_pool(base_col, j, col)
            from_all_users()
            from_user(base_mp, i, feat)

        def bit_of(b):
            return lax.rem(i // (1 << b), 2)

        def partner(b):
            return i + (1 << b) * (1 - 2 * bit_of(b))

        lows = [0]
        for b in range(bits):
            lows.append(lows[b] + bit_of(b) * (rows >> (b + 1)))

        def seg(b):
            size = rows >> b
            if b == 0:
                return pl.ds(0, rows)
            return pl.ds(pl.multiple_of(lows[b], size), size)

        def other(b):
            size = rows >> (b + 1)
            low = lows[b] + (1 - bit_of(b)) * size
            return pl.ds(pl.multiple_of(low, size), size)

        last = bits - 1

        def scatter_copy(c, b):
            rng = other(b) if b < last else seg(b)
            size = rows >> min(b + 1, last)
            return remote(
                send1.at[c, rng, :], recv1.at[b, c, pl.ds(0, size), :], a_ss.at[b, c], a_rs.at[b, c], {"mp": partner(b)}
            )

        def gather_copy(c, b):
            return remote(
                cross1.at[c, seg(b + 1), :], cross1.at[c, seg(b + 1), :], g_ss.at[b, c], g_rs.at[b, c], {"mp": partner(b)}
            )

        def gather_wait(c, b):
            remote(
                cross1.at[c, other(b), :], cross1.at[c, other(b), :], g_ss.at[b, c], g_rs.at[b, c], {"mp": partner(b)}
            ).wait_recv()

        def stage_a(c):
            w1_copies[c].wait()
            term = jnp.dot(base_mp[...], w1_v[c], preferred_element_type=F32)
            acc1[c] = term
            send1[c] = term.astype(BF16)
            copy = scatter_copy(c, 0)
            copy.start()
            pending.append(copy)

        def stage_b(c):
            for b in range(last):
                scatter_copy(c, b).wait_recv()
                size = rows >> (b + 1)
                term = acc1[c, seg(b + 1), :] + recv1[b, c, 0:size, :].astype(F32)
                if b + 1 < last:
                    acc1[c, seg(b + 1), :] = term
                send1[c, seg(b + 1), :] = term.astype(BF16)
                copy = scatter_copy(c, b + 1)
                copy.start()
                pending.append(copy)

        def stage_c(c):
            scatter_copy(c, last).wait_recv()
            size = rows >> last
            total = send1[c, seg(last), :].astype(F32) + recv1[last, c, 0:size, :].astype(F32)
            cols = slice(c * cw1, (c + 1) * cw1)
            base = base_col[seg(last), cols].astype(F32)
            cross1[c, seg(last), :] = (base * (total + b1_ref[:, cols]) + base).astype(BF16)
            if last > 0:
                copy = gather_copy(c, last - 1)
                copy.start()
                pending.append(copy)

        def line_copy(n, right, first):
            src = (q_send if first else (l_send if right else r_send)).at[n]
            if right:
                return remote(src, l_recv.at[n], l_ss.at[n], l_rs.at[n], {"cand": j + 1})
            return remote(src, r_recv.at[n], r_ss.at[n], r_rs.at[n], {"cand": j - 1})

        def stage_d(c):
            for b in range(last - 1, -1, -1):
                gather_wait(c, b)
                if b > 0:
                    copy = gather_copy(c, b - 1)
                    copy.start()
                    pending.append(copy)
            w2_copies[c].wait()
            for n in range(n2):
                cols = slice(n * cw2, (n + 1) * cw2)
                term = jnp.dot(
                    cross1[c], w2_v[c * cw1 : (c + 1) * cw1, cols], preferred_element_type=F32
                )
                if c > 0:
                    term = acc2[:, cols] + term
                if c < n1 - 1:
                    acc2[:, cols] = term
                    continue
                owner = (j == i * ratio + (n * cw2) // col).astype(F32)
                inner = (n * cw2) % col
                carried = cross1[inner // cw1, :, inner % cw1 : inner % cw1 + cw2].astype(F32)
                term = base_mp[:, cols].astype(F32) * (term + owner * b2_ref[:, cols]) + owner * carried
                q_send[n] = term.astype(BF16)

                @pl.when(j == 0)
                def _():
                    line_copy(n, True, True).start()

                @pl.when(j == n_cand - 1)
                def _():
                    line_copy(n, False, True).start()

        order = []
        for s in range(n1 + 1):
            if s < n1:
                order.append((stage_a, s))
            if s >= 1:
                order.append((stage_b, s - 1))
        for s in range(n1 + 1):
            if s < n1:
                order.append((stage_c, s))
            if s >= 1:
                order.append((stage_d, s - 1))
        started = False
        for stage, c in order:
            if stage is stage_c and c == 0:
                @pl.when(jnp.logical_not(user_side))
                def _():
                    from_pool(base_col, j, col)
                    from_all_users()

                from_user(base_col, j, col)
                for copy in small_copies[2:]:
                    copy.wait()
            stage(c)
            if stage is stage_a and c == n1 - 1:
                for copy in w2_copies:
                    copy.start()
            if stage is stage_c and not started:
                started = True
                for copy in w3_copies:
                    copy.start()

        def forward(n, right):
            came = (l_recv if right else r_recv)[n].astype(F32)
            (l_send if right else r_send)[n] = (came + q_send[n].astype(F32)).astype(BF16)
            line_copy(n, right, False).start()

        def take(n, right):
            if right:
                remote(l_send.at[n], l_recv.at[n], l_ss.at[n], l_rs.at[n], {"cand": j}).wait_recv()
            else:
                remote(r_send.at[n], r_recv.at[n], r_ss.at[n], r_rs.at[n], {"cand": j}).wait_recv()

        def third(n):
            w3_copies[n].wait()
            for p in range(n1):
                cols = slice(p * cw1, (p + 1) * cw1)
                term = jnp.dot(
                    x3[:, n * cw2 : (n + 1) * cw2], w3_v[n * cw2 : (n + 1) * cw2, cols], preferred_element_type=F32
                )
                if n > 0:
                    term = acc3[:, cols] + term
                acc3[:, cols] = term

        skew = min(3, n2)
        near_left = j < (n_cand + 1) // 2
        inner_device = jnp.logical_and(j > 0, j < n_cand - 1)
        for s in range(n2 + skew):
            if s < n2:
                @pl.when(jnp.logical_and(inner_device, near_left))
                def _():
                    take(s, True)
                    forward(s, True)

                @pl.when(jnp.logical_and(inner_device, jnp.logical_not(near_left)))
                def _():
                    take(s, False)
                    forward(s, False)

            n = s - skew
            if n < 0:
                continue

            @pl.when(jnp.logical_and(inner_device, near_left))
            def _():
                take(n, False)
                forward(n, False)

            @pl.when(jnp.logical_and(inner_device, jnp.logical_not(near_left)))
            def _():
                take(n, True)
                forward(n, True)

            cols = slice(n * cw2, (n + 1) * cw2)

            @pl.when(inner_device)
            def _():
                x3[:, cols] = (
                    q_send[n].astype(F32) + l_recv[n].astype(F32) + r_recv[n].astype(F32)
                ).astype(BF16)

            @pl.when(j == 0)
            def _():
                take(n, False)
                x3[:, cols] = (q_send[n].astype(F32) + r_recv[n].astype(F32)).astype(BF16)

            @pl.when(j == n_cand - 1)
            def _():
                take(n, True)
                x3[:, cols] = (q_send[n].astype(F32) + l_recv[n].astype(F32)).astype(BF16)

            third(n)

        def last_copy(c, b):
            size = rows >> (b + 1)
            return remote(
                send3.at[c, other(b), :], recv3.at[b, c, pl.ds(0, size), :], c_ss.at[b, c], c_rs.at[b, c], {"mp": partner(b)}
            )

        owner = (i == j // ratio).astype(F32)
        lanes = jnp.zeros((rows, 128), F32)
        for c in range(n1):
            cols = slice(c * cw1, (c + 1) * cw1)
            if ratio == 1:
                carried = x3[:, cols]
            else:
                carried = x3[:, pl.ds(pl.multiple_of(lax.rem(j, ratio) * col + c * cw1, 128), cw1)]
            term = (
                base_col[:, cols].astype(F32) * (acc3[:, cols] + owner * b3_ref[:, cols])
                + owner * carried.astype(F32)
            )
            acc3[:, cols] = term
            send3[c] = term.astype(BF16)
            copy = last_copy(c, 0)
            copy.start()
            pending.append(copy)
            scored = term * score_ref[cols].astype(F32).reshape(1, cw1)
            for k in range(0, cw1, 128):
                lanes = lanes + scored[:, k : k + 128]
        q_rows[...] = jnp.zeros_like(q_rows)
        q_rows[0:rows, :] = lanes
        q_all[me] = jnp.sum(q_rows[...].T, axis=0, keepdims=True)

        def q_copy(d):
            peer = lax.rem(me + d, group)
            return remote(
                q_all.at[me], q_all.at[me], q_ss.at[d], q_rs.at[me],
                {"mp": peer // n_cand, "cand": lax.rem(peer, n_cand)},
            )

        def q_start(d, carry):
            q_copy(d).start()
            return carry

        lax.fori_loop(1, group, q_start, 0)

        for b in range(bits):
            for c in range(n1):
                cols = slice(c * cw1, (c + 1) * cw1)
                last_copy(c, b).wait_recv()
                size = rows >> (b + 1)
                term = acc3[seg(b + 1), cols] + recv3[b, c, 0:size, :].astype(F32)
                if b + 1 < bits:
                    acc3[seg(b + 1), cols] = term
                    send3[c, seg(b + 1), :] = term.astype(BF16)
                    copy = last_copy(c, b + 1)
                    copy.start()
                    pending.append(copy)
                else:
                    out_ref[:, cols] = term.astype(BF16)

        def q_wait(d, carry):
            k = lax.rem(me - d + group, group)
            remote(q_all.at[k], q_all.at[k], q_ss.at[d], q_rs.at[k], {"cand": j}).wait_recv()
            return carry

        lax.fori_loop(1, group, q_wait, 0)
        total = jnp.sum(q_all[...], axis=0)
        for k in range(n_mp):
            p = reverse_bits(k, bits)

            @pl.when(i == k)
            def _():
                logit_ref[...] = total[:, p * block : (p + 1) * block]

        for copy in pending:
            copy.wait_send()
        for d in range(1, n_cand):
            user_copy(d).wait_send()

        def q_sent(d, carry):
            q_copy(d).wait_send()
            return carry

        lax.fori_loop(1, group, q_sent, 0)
        for n in range(n2):
            @pl.when(j < n_cand - 1)
            def _():
                line_copy(n, True, False).wait_send()

            @pl.when(j > 0)
            def _():
                line_copy(n, False, False).wait_send()

    return kernel


def solution(mesh):
    n_mp, n_cand = mesh.shape["mp"], mesh.shape["cand"]

    def body(
        user_feats, user_slot, cand_pool, cand_ids, first_weight, first_bias,
        second_weight, second_bias, third_weight, third_bias, score_weight,
    ):
        slots_each, half_width = user_feats.shape
        users, per_user = cand_ids.shape
        rows = users * per_user
        pool_count = cand_pool.shape[0]
        feat, col = first_weight.shape
        n1 = max(1, col // 512)
        n2 = max(1, feat // 256)
        cw1, cw2 = col // n1, feat // n2
        bits = n_mp.bit_length() - 1
        block = rows // n_mp
        group = n_mp * n_cand
        shapes = (rows, per_user, users, slots_each, half_width, pool_count, feat, col, n1, n2)
        vmem = pl.BlockSpec(memory_space=pltpu.VMEM)
        smem = pl.BlockSpec(memory_space=pltpu.SMEM)
        hbm = pl.BlockSpec(memory_space=pl.ANY)
        dma = pltpu.SemaphoreType.DMA
        exchange = rows >> (1 if bits > 1 else 0)
        crossed, logits = pl.pallas_call(
            make_kernel(n_mp, n_cand, shapes),
            out_shape=(
                pltpu.VMEM((block, col), BF16),
                pltpu.VMEM((1, block), F32),
            ),
            in_specs=[hbm, smem] + [hbm] * 9,
            out_specs=(vmem, vmem),
            scratch_shapes=[
                pltpu.VMEM((slots_each, half_width), BF16),
                pltpu.VMEM((users, per_user), jnp.int32),
                pltpu.VMEM((1, col), F32),
                pltpu.VMEM((1, feat), F32),
                pltpu.VMEM((1, col), F32),
                pltpu.VMEM((col,), BF16),
                dma((6,)),
                pltpu.VMEM((n_cand, slots_each, half_width), BF16),
                pltpu.VMEM((pool_count, half_width), BF16),
                pltpu.VMEM((n1, feat, cw1), BF16),
                pltpu.VMEM((col, feat), BF16),
                pltpu.VMEM((feat, col), BF16),
                pltpu.VMEM((rows, pool_count), BF16),
                pltpu.VMEM((rows, feat), BF16),
                pltpu.VMEM((rows, col), BF16),
                pltpu.VMEM((n1, rows, cw1), F32),
                pltpu.VMEM((n1, rows, cw1), BF16),
                pltpu.VMEM((bits, n1, exchange, cw1), BF16),
                pltpu.VMEM((n1, rows, cw1), BF16),
                pltpu.VMEM((rows, feat), F32),
                pltpu.VMEM((n2, rows, cw2), BF16),
                pltpu.VMEM((n2, rows, cw2), BF16),
                pltpu.VMEM((n2, rows, cw2), BF16),
                pltpu.VMEM((n2, rows, cw2), BF16),
                pltpu.VMEM((n2, rows, cw2), BF16),
                pltpu.VMEM((rows, feat), BF16),
                pltpu.VMEM((rows, col), F32),
                pltpu.VMEM((n1, rows, cw1), BF16),
                pltpu.VMEM((bits, n1, rows // 2, cw1), BF16),
                pltpu.VMEM((max(rows, 128), 128), F32),
                pltpu.VMEM((group, 1, max(rows, 128)), F32),
                dma((1 + 2 * n1 + n2,)),
                dma((n_cand,)),
                dma((n_cand,)),
                dma((bits, n1)),
                dma((bits, n1)),
                dma((bits, n1)),
                dma((bits, n1)),
                dma((n2,)),
                dma((n2,)),
                dma((n2,)),
                dma((n2,)),
                dma((bits, n1)),
                dma((bits, n1)),
                dma((group,)),
                dma((group,)),
            ],
            compiler_params=pltpu.CompilerParams(
                collective_id=0, has_side_effects=True, vmem_limit_bytes=67043328 - 3000 * 1024
            ),
        )(
            user_feats, user_slot, cand_pool, cand_ids, first_weight, first_bias.reshape(1, -1),
            second_weight, second_bias.reshape(1, -1), third_weight, third_bias.reshape(1, -1),
            score_weight,
        )
        crossed, logits = pl.pallas_call(
            hand_on,
            out_shape=(
                jax.ShapeDtypeStruct((block, col), BF16),
                jax.ShapeDtypeStruct((1, block), F32),
            ),
            in_specs=[vmem, vmem],
            out_specs=(hbm, hbm),
            scratch_shapes=[dma((2,))],
            compiler_params=pltpu.CompilerParams(vmem_limit_bytes=1024 * 1024),
        )(crossed, logits)
        return crossed, logits.reshape(-1)

    in_specs = (
        P(("groups", "cand"), None),
        P("groups"),
        P("groups", None),
        P("groups", None),
        P("mp", "cand"),
        P("cand"),
        P("cand", "mp"),
        P("mp"),
        P("mp", "cand"),
        P("cand"),
        P("cand"),
    )
    out_specs = (P(("groups", "mp"), "cand"), P(("groups", "mp")))
    return jax.shard_map(body, mesh=mesh, in_specs=in_specs, out_specs=out_specs, check_vma=False)
```

```python
import jax
import jax.numpy as jnp
from jax import lax
from jax.experimental import pallas as pl
from jax.experimental.pallas import tpu as pltpu
from jax.sharding import PartitionSpec as P

MESH = pl.DeviceIdType.MESH
F32 = jnp.float32
BF16 = jnp.bfloat16


def reverse_bits(value, bits):
    out = 0
    for _ in range(bits):
        out = 2 * out + value % 2
        value //= 2
    return out


def hand_on(crossed_ref, logit_ref, crossed_hbm, logit_hbm, sem):
    copies = [
        pltpu.make_async_copy(crossed_ref, crossed_hbm, sem.at[0]),
        pltpu.make_async_copy(logit_ref, logit_hbm, sem.at[1]),
    ]
    for copy in copies:
        copy.start()
    for copy in copies:
        copy.wait()


def make_kernel(n_mp, n_cand, shapes):
    rows, per_user, users, slots_each, half_width, pool_count, feat, col, n1, n2 = shapes
    cw1, cw2 = col // n1, feat // n2
    bits = n_mp.bit_length() - 1
    block = rows // n_mp
    ratio = feat // col
    group = n_mp * n_cand

    def kernel(
        user_hbm, slot_ref, pool_hbm, ids_hbm, w1_hbm, b1_hbm, w2_hbm, b2_hbm, w3_hbm, b3_hbm, score_hbm,
        out_ref, logit_ref,
        user_ref, ids_ref, b1_ref, b2_ref, b3_ref, score_ref, small_sem, slots, pool_v, w1_v, w2_v, w3_v, onehot, base_mp, base_col,
        acc1, send1, recv1, cross1, acc2, q_send, l_recv, r_recv, l_send, r_send, x3, acc3, send3, recv3, q_rows, q_all,
        w_sem, user_ss, user_rs, a_ss, a_rs, g_ss, g_rs, l_ss, l_rs, r_ss, r_rs, c_ss, c_rs, q_ss, q_rs,
    ):
        i = lax.axis_index("mp")
        j = lax.axis_index("cand")
        me = i * n_cand + j
        pending = []

        def remote(src, dst, ss, rs, where):
            return pltpu.make_async_remote_copy(
                src_ref=src, dst_ref=dst, send_sem=ss, recv_sem=rs, device_id=where, device_id_type=MESH
            )

        small_copies = [
            pltpu.make_async_copy(src, dst, small_sem.at[k])
            for k, (src, dst) in enumerate(
                (
                    (user_hbm, user_ref), (ids_hbm, ids_ref), (b1_hbm, b1_ref),
                    (b2_hbm, b2_ref), (b3_hbm, b3_ref), (score_hbm, score_ref),
                )
            )
        ]
        for copy in small_copies:
            copy.start()
        barrier = pltpu.get_barrier_semaphore()

        def greet(d, carry):
            peer = lax.rem(me + d, group)
            pl.semaphore_signal(
                barrier, inc=1, device_id={"mp": peer // n_cand, "cand": lax.rem(peer, n_cand)}, device_id_type=MESH
            )
            return carry

        lax.fori_loop(1, group, greet, 0)

        pool_copy = pltpu.make_async_copy(pool_hbm, pool_v, w_sem.at[0])
        w1_copies = [
            pltpu.make_async_copy(w1_hbm.at[:, pl.ds(c * cw1, cw1)], w1_v.at[c], w_sem.at[1 + c]) for c in range(n1)
        ]
        w2_copies = [
            pltpu.make_async_copy(w2_hbm.at[pl.ds(c * cw1, cw1), :], w2_v.at[pl.ds(c * cw1, cw1), :], w_sem.at[1 + n1 + c])
            for c in range(n1)
        ]
        w3_copies = [
            pltpu.make_async_copy(w3_hbm.at[pl.ds(c * cw2, cw2), :], w3_v.at[pl.ds(c * cw2, cw2), :], w_sem.at[1 + 2 * n1 + c])
            for c in range(n2)
        ]
        pool_copy.start()
        for copy in w1_copies:
            copy.start()

        small_copies[0].wait()
        pl.semaphore_wait(barrier, group - 1)

        def user_copy(d):
            return remote(
                user_ref, slots.at[j], user_ss.at[d - 1], user_rs.at[j], {"cand": lax.rem(j + d, n_cand)}
            )

        for d in range(1, n_cand):
            user_copy(d).start()
        slots[j] = user_ref[...]
        small_copies[1].wait()

        for u in range(users):
            hot = (
                lax.broadcasted_iota(jnp.int32, (pool_count, per_user), 0) == ids_ref[u : u + 1, :]
            ).astype(F32).T
            for p in range(n_mp):
                first = reverse_bits(p, bits) * block
                if first // per_user == u:
                    off = first % per_user
                    onehot[p * block : (p + 1) * block, :] = hot[off : off + block].astype(BF16)

        def from_pool(dst, index, width):
            @pl.when(index >= half_width // width)
            def _():
                for c in range(0, width, 256):
                    start = pl.multiple_of(index * width - half_width + c, 128)
                    dst[:, c : c + 256] = jnp.dot(
                        onehot[...], pool_v[:, pl.ds(start, 256)], preferred_element_type=F32
                    ).astype(BF16)

        def from_user(dst, index, width):
            @pl.when(index < half_width // width)
            def _():
                start = pl.multiple_of(index * width, 128)
                for p in range(n_mp):
                    slot = slot_ref[(reverse_bits(p, bits) * block) // per_user]
                    row = slots[slot // slots_each, :, pl.ds(start, width)].astype(F32)
                    if slots_each > 1:
                        pick = lax.broadcasted_iota(jnp.int32, row.shape, 0) == lax.rem(slot, slots_each)
                        row = jnp.sum(jnp.where(pick, row, 0.0), axis=0, keepdims=True)
                    dst[p * block : (p + 1) * block, :] = jnp.broadcast_to(row, (block, width)).astype(BF16)

        def from_all_users():
            for d in range(1, n_cand):
                k = lax.rem(j - d + n_cand, n_cand)
                remote(user_ref, slots.at[k], user_ss.at[d - 1], user_rs.at[k], {"cand": k}).wait_recv()

        pool_copy.wait()
        from_pool(base_mp, i, feat)
        user_side = i < half_width // feat

        @pl.when(user_side)
        def _():
            from_pool(base_col, j, col)
            from_all_users()
            from_user(base_mp, i, feat)

        def bit_of(b):
            return lax.rem(i // (1 << b), 2)

        def partner(b):
            return i + (1 << b) * (1 - 2 * bit_of(b))

        lows = [0]
        for b in range(bits):
            lows.append(lows[b] + bit_of(b) * (rows >> (b + 1)))

        def seg(b):
            size = rows >> b
            if b == 0:
                return pl.ds(0, rows)
            return pl.ds(pl.multiple_of(lows[b], size), size)

        def other(b):
            size = rows >> (b + 1)
            low = lows[b] + (1 - bit_of(b)) * size
            return pl.ds(pl.multiple_of(low, size), size)

        last = bits - 1

        def scatter_copy(c, b):
            rng = other(b) if b < last else seg(b)
            size = rows >> min(b + 1, last)
            return remote(
                send1.at[c, rng, :], recv1.at[b, c, pl.ds(0, size), :], a_ss.at[b, c], a_rs.at[b, c], {"mp": partner(b)}
            )

        def gather_copy(c, b):
            return remote(
                cross1.at[c, seg(b + 1), :], cross1.at[c, seg(b + 1), :], g_ss.at[b, c], g_rs.at[b, c], {"mp": partner(b)}
            )

        def gather_wait(c, b):
            remote(
                cross1.at[c, other(b), :], cross1.at[c, other(b), :], g_ss.at[b, c], g_rs.at[b, c], {"mp": partner(b)}
            ).wait_recv()

        def stage_a(c):
            w1_copies[c].wait()
            term = jnp.dot(base_mp[...], w1_v[c], preferred_element_type=F32)
            acc1[c] = term
            send1[c] = term.astype(BF16)
            copy = scatter_copy(c, 0)
            copy.start()
            pending.append(copy)

        def stage_b(c):
            for b in range(last):
                scatter_copy(c, b).wait_recv()
                size = rows >> (b + 1)
                term = acc1[c, seg(b + 1), :] + recv1[b, c, 0:size, :].astype(F32)
                if b + 1 < last:
                    acc1[c, seg(b + 1), :] = term
                send1[c, seg(b + 1), :] = term.astype(BF16)
                copy = scatter_copy(c, b + 1)
                copy.start()
                pending.append(copy)

        def stage_c(c):
            scatter_copy(c, last).wait_recv()
            size = rows >> last
            total = send1[c, seg(last), :].astype(F32) + recv1[last, c, 0:size, :].astype(F32)
            cols = slice(c * cw1, (c + 1) * cw1)
            base = base_col[seg(last), cols].astype(F32)
            cross1[c, seg(last), :] = (base * (total + b1_ref[:, cols]) + base).astype(BF16)
            if last > 0:
                copy = gather_copy(c, last - 1)
                copy.start()
                pending.append(copy)

        def line_copy(n, right, first):
            src = (q_send if first else (l_send if right else r_send)).at[n]
            if right:
                return remote(src, l_recv.at[n], l_ss.at[n], l_rs.at[n], {"cand": j + 1})
            return remote(src, r_recv.at[n], r_ss.at[n], r_rs.at[n], {"cand": j - 1})

        def stage_d(c):
            for b in range(last - 1, -1, -1):
                gather_wait(c, b)
                if b > 0:
                    copy = gather_copy(c, b - 1)
                    copy.start()
                    pending.append(copy)
            w2_copies[c].wait()
            for n in range(n2):
                cols = slice(n * cw2, (n + 1) * cw2)
                term = jnp.dot(
                    cross1[c], w2_v[c * cw1 : (c + 1) * cw1, cols], preferred_element_type=F32
                )
                if c > 0:
                    term = acc2[:, cols] + term
                if c < n1 - 1:
                    acc2[:, cols] = term
                    continue
                owner = (j == i * ratio + (n * cw2) // col).astype(F32)
                inner = (n * cw2) % col
                carried = cross1[inner // cw1, :, inner % cw1 : inner % cw1 + cw2].astype(F32)
                term = base_mp[:, cols].astype(F32) * (term + owner * b2_ref[:, cols]) + owner * carried
                q_send[n] = term.astype(BF16)

                @pl.when(j == 0)
                def _():
                    line_copy(n, True, True).start()

                @pl.when(j == n_cand - 1)
                def _():
                    line_copy(n, False, True).start()

        order = []
        for s in range(n1 + 1):
            if s < n1:
                order.append((stage_a, s))
            if s >= 1:
                order.append((stage_b, s - 1))
        for s in range(n1 + 1):
            if s < n1:
                order.append((stage_c, s))
            if s >= 1:
                order.append((stage_d, s - 1))
        started = False
        for stage, c in order:
            if stage is stage_c and c == 0:
                @pl.when(jnp.logical_not(user_side))
                def _():
                    from_pool(base_col, j, col)
                    from_all_users()

                from_user(base_col, j, col)
                for copy in small_copies[2:]:
                    copy.wait()
            stage(c)
            if stage is stage_a and c == n1 - 1:
                for copy in w2_copies:
                    copy.start()
            if stage is stage_c and not started:
                started = True
                for copy in w3_copies:
                    copy.start()

        def forward(n, right):
            came = (l_recv if right else r_recv)[n].astype(F32)
            (l_send if right else r_send)[n] = (came + q_send[n].astype(F32)).astype(BF16)
            line_copy(n, right, False).start()

        def take(n, right):
            if right:
                remote(l_send.at[n], l_recv.at[n], l_ss.at[n], l_rs.at[n], {"cand": j}).wait_recv()
            else:
                remote(r_send.at[n], r_recv.at[n], r_ss.at[n], r_rs.at[n], {"cand": j}).wait_recv()

        def third(n):
            w3_copies[n].wait()
            for p in range(n1):
                cols = slice(p * cw1, (p + 1) * cw1)
                term = jnp.dot(
                    x3[:, n * cw2 : (n + 1) * cw2], w3_v[n * cw2 : (n + 1) * cw2, cols], preferred_element_type=F32
                )
                if n > 0:
                    term = acc3[:, cols] + term
                acc3[:, cols] = term

        skew = min(4, n2)
        near_left = j < (n_cand + 1) // 2
        inner_device = jnp.logical_and(j > 0, j < n_cand - 1)
        for s in range(n2 + skew):
            if s < n2:
                @pl.when(jnp.logical_and(inner_device, near_left))
                def _():
                    take(s, True)
                    forward(s, True)

                @pl.when(jnp.logical_and(inner_device, jnp.logical_not(near_left)))
                def _():
                    take(s, False)
                    forward(s, False)

            n = s - skew
            if n < 0:
                continue

            @pl.when(jnp.logical_and(inner_device, near_left))
            def _():
                take(n, False)
                forward(n, False)

            @pl.when(jnp.logical_and(inner_device, jnp.logical_not(near_left)))
            def _():
                take(n, True)
                forward(n, True)

            cols = slice(n * cw2, (n + 1) * cw2)

            @pl.when(inner_device)
            def _():
                x3[:, cols] = (
                    q_send[n].astype(F32) + l_recv[n].astype(F32) + r_recv[n].astype(F32)
                ).astype(BF16)

            @pl.when(j == 0)
            def _():
                take(n, False)
                x3[:, cols] = (q_send[n].astype(F32) + r_recv[n].astype(F32)).astype(BF16)

            @pl.when(j == n_cand - 1)
            def _():
                take(n, True)
                x3[:, cols] = (q_send[n].astype(F32) + l_recv[n].astype(F32)).astype(BF16)

            third(n)

        def last_copy(c, b):
            size = rows >> (b + 1)
            return remote(
                send3.at[c, other(b), :], recv3.at[b, c, pl.ds(0, size), :], c_ss.at[b, c], c_rs.at[b, c], {"mp": partner(b)}
            )

        owner = (i == j // ratio).astype(F32)
        lanes = jnp.zeros((rows, 128), F32)
        for c in range(n1):
            cols = slice(c * cw1, (c + 1) * cw1)
            if ratio == 1:
                carried = x3[:, cols]
            else:
                carried = x3[:, pl.ds(pl.multiple_of(lax.rem(j, ratio) * col + c * cw1, 128), cw1)]
            term = (
                base_col[:, cols].astype(F32) * (acc3[:, cols] + owner * b3_ref[:, cols])
                + owner * carried.astype(F32)
            )
            acc3[:, cols] = term
            send3[c] = term.astype(BF16)
            copy = last_copy(c, 0)
            copy.start()
            pending.append(copy)
            scored = term * score_ref[cols].astype(F32).reshape(1, cw1)
            for k in range(0, cw1, 128):
                lanes = lanes + scored[:, k : k + 128]
        q_rows[...] = jnp.zeros_like(q_rows)
        q_rows[0:rows, :] = lanes
        q_all[me] = jnp.sum(q_rows[...].T, axis=0, keepdims=True)

        def q_copy(d):
            peer = lax.rem(me + d, group)
            return remote(
                q_all.at[me], q_all.at[me], q_ss.at[d], q_rs.at[me],
                {"mp": peer // n_cand, "cand": lax.rem(peer, n_cand)},
            )

        def q_start(d, carry):
            q_copy(d).start()
            return carry

        lax.fori_loop(1, group, q_start, 0)

        for b in range(bits):
            for c in range(n1):
                cols = slice(c * cw1, (c + 1) * cw1)
                last_copy(c, b).wait_recv()
                size = rows >> (b + 1)
                term = acc3[seg(b + 1), cols] + recv3[b, c, 0:size, :].astype(F32)
                if b + 1 < bits:
                    acc3[seg(b + 1), cols] = term
                    send3[c, seg(b + 1), :] = term.astype(BF16)
                    copy = last_copy(c, b + 1)
                    copy.start()
                    pending.append(copy)
                else:
                    out_ref[:, cols] = term.astype(BF16)

        def q_wait(d, carry):
            k = lax.rem(me - d + group, group)
            remote(q_all.at[k], q_all.at[k], q_ss.at[d], q_rs.at[k], {"cand": j}).wait_recv()
            return carry

        lax.fori_loop(1, group, q_wait, 0)
        total = jnp.sum(q_all[...], axis=0)
        for k in range(n_mp):
            p = reverse_bits(k, bits)

            @pl.when(i == k)
            def _():
                logit_ref[...] = total[:, p * block : (p + 1) * block]

        for copy in pending:
            copy.wait_send()
        for d in range(1, n_cand):
            user_copy(d).wait_send()

        def q_sent(d, carry):
            q_copy(d).wait_send()
            return carry

        lax.fori_loop(1, group, q_sent, 0)
        for n in range(n2):
            @pl.when(j < n_cand - 1)
            def _():
                line_copy(n, True, False).wait_send()

            @pl.when(j > 0)
            def _():
                line_copy(n, False, False).wait_send()

    return kernel


def solution(mesh):
    n_mp, n_cand = mesh.shape["mp"], mesh.shape["cand"]

    def body(
        user_feats, user_slot, cand_pool, cand_ids, first_weight, first_bias,
        second_weight, second_bias, third_weight, third_bias, score_weight,
    ):
        slots_each, half_width = user_feats.shape
        users, per_user = cand_ids.shape
        rows = users * per_user
        pool_count = cand_pool.shape[0]
        feat, col = first_weight.shape
        n1 = max(1, col // 512)
        n2 = max(1, feat // 256)
        cw1, cw2 = col // n1, feat // n2
        bits = n_mp.bit_length() - 1
        block = rows // n_mp
        group = n_mp * n_cand
        shapes = (rows, per_user, users, slots_each, half_width, pool_count, feat, col, n1, n2)
        vmem = pl.BlockSpec(memory_space=pltpu.VMEM)
        smem = pl.BlockSpec(memory_space=pltpu.SMEM)
        hbm = pl.BlockSpec(memory_space=pl.ANY)
        dma = pltpu.SemaphoreType.DMA
        exchange = rows >> (1 if bits > 1 else 0)
        crossed, logits = pl.pallas_call(
            make_kernel(n_mp, n_cand, shapes),
            out_shape=(
                pltpu.VMEM((block, col), BF16),
                pltpu.VMEM((1, block), F32),
            ),
            in_specs=[hbm, smem] + [hbm] * 9,
            out_specs=(vmem, vmem),
            scratch_shapes=[
                pltpu.VMEM((slots_each, half_width), BF16),
                pltpu.VMEM((users, per_user), jnp.int32),
                pltpu.VMEM((1, col), F32),
                pltpu.VMEM((1, feat), F32),
                pltpu.VMEM((1, col), F32),
                pltpu.VMEM((col,), BF16),
                dma((6,)),
                pltpu.VMEM((n_cand, slots_each, half_width), BF16),
                pltpu.VMEM((pool_count, half_width), BF16),
                pltpu.VMEM((n1, feat, cw1), BF16),
                pltpu.VMEM((col, feat), BF16),
                pltpu.VMEM((feat, col), BF16),
                pltpu.VMEM((rows, pool_count), BF16),
                pltpu.VMEM((rows, feat), BF16),
                pltpu.VMEM((rows, col), BF16),
                pltpu.VMEM((n1, rows, cw1), F32),
                pltpu.VMEM((n1, rows, cw1), BF16),
                pltpu.VMEM((bits, n1, exchange, cw1), BF16),
                pltpu.VMEM((n1, rows, cw1), BF16),
                pltpu.VMEM((rows, feat), F32),
                pltpu.VMEM((n2, rows, cw2), BF16),
                pltpu.VMEM((n2, rows, cw2), BF16),
                pltpu.VMEM((n2, rows, cw2), BF16),
                pltpu.VMEM((n2, rows, cw2), BF16),
                pltpu.VMEM((n2, rows, cw2), BF16),
                pltpu.VMEM((rows, feat), BF16),
                pltpu.VMEM((rows, col), F32),
                pltpu.VMEM((n1, rows, cw1), BF16),
                pltpu.VMEM((bits, n1, rows // 2, cw1), BF16),
                pltpu.VMEM((max(rows, 128), 128), F32),
                pltpu.VMEM((group, 1, max(rows, 128)), F32),
                dma((1 + 2 * n1 + n2,)),
                dma((n_cand,)),
                dma((n_cand,)),
                dma((bits, n1)),
                dma((bits, n1)),
                dma((bits, n1)),
                dma((bits, n1)),
                dma((n2,)),
                dma((n2,)),
                dma((n2,)),
                dma((n2,)),
                dma((bits, n1)),
                dma((bits, n1)),
                dma((group,)),
                dma((group,)),
            ],
            compiler_params=pltpu.CompilerParams(
                collective_id=0, has_side_effects=True, vmem_limit_bytes=67043328 - 3000 * 1024
            ),
        )(
            user_feats, user_slot, cand_pool, cand_ids, first_weight, first_bias.reshape(1, -1),
            second_weight, second_bias.reshape(1, -1), third_weight, third_bias.reshape(1, -1),
            score_weight,
        )
        crossed, logits = pl.pallas_call(
            hand_on,
            out_shape=(
                jax.ShapeDtypeStruct((block, col), BF16),
                jax.ShapeDtypeStruct((1, block), F32),
            ),
            in_specs=[vmem, vmem],
            out_specs=(hbm, hbm),
            scratch_shapes=[dma((2,))],
            compiler_params=pltpu.CompilerParams(vmem_limit_bytes=1024 * 1024),
        )(crossed, logits)
        return crossed, logits.reshape(-1)

    in_specs = (
        P(("groups", "cand"), None),
        P("groups"),
        P("groups", None),
        P("groups", None),
        P("mp", "cand"),
        P("cand"),
        P("cand", "mp"),
        P("mp"),
        P("mp", "cand"),
        P("cand"),
        P("cand"),
    )
    out_specs = (P(("groups", "mp"), "cand"), P(("groups", "mp")))
    return jax.shard_map(body, mesh=mesh, in_specs=in_specs, out_specs=out_specs, check_vma=False)
```
